32 devices in a mesh: grp: 4 (over z), dev: 8 (over y, x, core).
Axes of the slice: x: 2, y: 2, z: 4, core: 2. Of those that a mesh axis runs over, the one named last changes fastest.
Arguments:
- amounts: float32 [64, 524288], P('dev', 'grp'), may hold values from -0.06 to 0.06, as said below
Outputs:
- offsets: float32 [64, 524288], P(None, ('grp', 'dev'))
The draws below stay inside these ranges and needn't reach their ends.
Inputs may be any that keep to these rules, and one draw needn't show every extreme that they name: `amounts`: each entry lies within 0.06 of zero.
All inputs are finite; a program needn't handle non-finite values.
Results may differ from the reference program's by a relative error of at most 0.00095.
Values sent between devices are 32-bit elements; how exact they have to be, the bound alone decides.
No kernel may reach another device: no remote copies, remote signals or barrier semaphores. Data moves between devices by JAX's collectives and lax.ppermute only.
A program may use at most 64 MiB of HBM per device.

```python
import jax
import jax.numpy as jnp

COLS = 64
ROW_DEV = 16384
ROWS = 524288


def draw_amounts(key, part):
    subkeys = jax.random.split(jax.random.fold_in(key, 17), 3)
    regions = ROWS // (ROW_DEV // 4)
    noise = jax.random.uniform(subkeys[0], (COLS, ROWS + 1), jnp.float32, -1.0, 1.0)
    reach = 1.0
    drift = jax.random.uniform(subkeys[2], (COLS, 1), jnp.float32, 0.0, 2.0)
    factor = jnp.exp(jax.random.uniform(subkeys[1], (COLS, regions), jnp.float32, -reach, reach))
    factor = jnp.repeat(factor, ROW_DEV // 4, axis=1, total_repeat_length=ROWS)
    rough = 0.01 * (noise[:, 1:] - noise[:, :-1])
    values = factor * (rough + drift / ROWS)
    return values.astype(jnp.float32)


def setup_inputs(seed: int = 0) -> dict:
    arg_keys = jax.random.split(jax.random.key(seed), 2)
    amounts = draw_amounts(jax.random.fold_in(arg_keys[1], 71), 0)
    return {"amounts": amounts}


def exclusive_rows(values, block_len):
    chans, length = values.shape
    blocks = values.reshape(chans, length // block_len, block_len)
    within = jnp.cumsum(blocks, axis=2) - blocks
    sums = jnp.sum(blocks, axis=2)
    starts = jnp.cumsum(sums, axis=1) - sums
    return (within + starts[:, :, None]).reshape(chans, length)


def reference(amounts):
    return exclusive_rows(amounts, 512)
```

```python
import functools

import jax
import jax.numpy as jnp
from jax import lax
from jax.experimental import pallas as pl
from jax.experimental.pallas import tpu as pltpu
from jax.sharding import PartitionSpec as P

LANES = 128
VMEM = pl.BlockSpec(memory_space=pltpu.VMEM)
HBM = pl.BlockSpec(memory_space=pltpu.HBM)


def params(mib, flops):
    return {
        "compiler_params": pltpu.CompilerParams(vmem_limit_bytes=mib << 20),
        "cost_estimate": pl.CostEstimate(flops=flops, bytes_accessed=0, transcendentals=0),
    }


def shape(*dims):
    return jax.ShapeDtypeStruct(dims, jnp.float32)


def swap(value, k):
    count = lax.axis_size("dev")
    return lax.ppermute(value, "dev", [(i, i ^ k) for i in range(count)])


def shift_later(value, by):
    count = lax.axis_size("grp")
    return lax.ppermute(value, "grp", [(i, i + by) for i in range(count - by)])


def grab_kernel(ks, rows, a_ref, *refs):
    outs, sems = refs[: len(ks)], refs[-1]
    me = lax.axis_index("dev")
    copies = []
    for n, k in enumerate(ks):
        start = pl.multiple_of((me ^ k) * rows, rows)
        copy = pltpu.make_async_copy(a_ref.at[:, pl.ds(start, rows)], outs[n], sems.at[n])
        copy.start()
        copies.append(copy)
    for copy in copies:
        copy.wait()


def grab(a, ks, rows):
    chans = a.shape[0]
    return pl.pallas_call(
        functools.partial(grab_kernel, ks, rows),
        out_shape=[shape(chans, rows)] * len(ks),
        in_specs=[HBM],
        out_specs=[VMEM] * len(ks),
        scratch_shapes=[pltpu.SemaphoreType.DMA((len(ks),))],
        name="grab",
        **params(4, 1000000),
    )(a)


def piece_sum(ref):
    chans, rows = ref.shape
    width = 8 * LANES

    def step(n, acc):
        at = pl.multiple_of(n * width, width)
        return acc + ref[:, pl.ds(at, width)]

    acc = lax.fori_loop(1, rows // width, step, ref[:, :width], unroll=True)
    total = acc[:, :LANES]
    for n in range(1, 8):
        total = total + acc[:, n * LANES : (n + 1) * LANES]
    return jnp.broadcast_to(jnp.sum(total, axis=1, keepdims=True), (chans, LANES))


def sums_kernel(early, late, rows, a_ref, *refs):
    early_refs = refs[: len(early)]
    late_refs = refs[len(early) : len(early) + len(late)]
    total_ref, sums_ref, sems = refs[len(early) + len(late) :]
    me = lax.axis_index("dev")
    chans = a_ref.shape[0]
    copies = []
    for n, k in enumerate(late):
        start = pl.multiple_of((me ^ k) * rows, rows)
        copy = pltpu.make_async_copy(a_ref.at[:, pl.ds(start, rows)], late_refs[n], sems.at[n])
        copy.start()
        copies.append(copy)
    total = jnp.zeros((chans, LANES), jnp.float32)
    for n, k in enumerate(early + late):
        if n >= len(early):
            copies[n - len(early)].wait()
        part = piece_sum(early_refs[n] if n < len(early) else late_refs[n - len(early)])
        total = total + part
        sums_ref[pl.ds(pl.multiple_of((me ^ k) * chans, chans), chans), :] = part
    total_ref[...] = total


def sums(a, early, early_pieces, late, rows):
    chans, length = a.shape
    return pl.pallas_call(
        functools.partial(sums_kernel, early, late, rows),
        out_shape=[shape(chans, rows)] * len(late)
        + [shape(chans, LANES), shape(chans * (length // rows), LANES)],
        in_specs=[HBM] + [VMEM] * len(early),
        out_specs=[VMEM] * (len(late) + 2),
        scratch_shapes=[pltpu.SemaphoreType.DMA((len(late),))],
        name="sums",
        **params(8, 40000000),
    )(a, *early_pieces)


def carry_kernel(apart, inside, shifts, sums_ref, *refs):
    group_refs, refs = refs[:shifts], refs[shifts:]
    old_refs, refs = refs[: len(inside)], refs[len(inside) :]
    new_refs, apart_refs, carry_ref = refs[: len(inside)], refs[len(inside) : -1], refs[-1]
    me = lax.axis_index("dev")
    chans = group_refs[0].shape[0]
    count = sums_ref.shape[0] // chans
    carry = jnp.zeros((chans, LANES), jnp.float32)
    for ref in group_refs:
        carry = carry + ref[...]
    for e in range(count):
        carry_ref[e * chans : (e + 1) * chans, :] = carry
        carry = carry + sums_ref[e * chans : (e + 1) * chans, :]

    def carry_of(k):
        return carry_ref[pl.ds(pl.multiple_of((me ^ k) * chans, chans), chans), :]

    lane = lax.broadcasted_iota(jnp.int32, (chans, LANES), 1)
    for n, k in enumerate(inside):
        last = old_refs[n].shape[1] - LANES
        new_refs[n][:, last:] = jnp.where(lane == LANES - 1, carry_of(k), old_refs[n][:, last:])
    for n, k in enumerate(apart):
        apart_refs[n][...] = carry_of(k)


def carries(chunk_sums, groups, inside, pieces, apart):
    chans, rows = pieces[0].shape
    return pl.pallas_call(
        functools.partial(carry_kernel, apart, inside, len(groups)),
        out_shape=[shape(chans, rows)] * len(inside) + [shape(chans, LANES)] * len(apart),
        in_specs=[VMEM] * (1 + len(groups) + len(inside)),
        out_specs=[VMEM] * (len(inside) + len(apart)),
        scratch_shapes=[pltpu.VMEM(chunk_sums.shape, jnp.float32)],
        input_output_aliases={1 + len(groups) + n: n for n in range(len(inside))},
        name="carries",
        **params(8, 10000000),
    )(chunk_sums, *groups, *pieces)


def scan_piece(piece_ref, carry, out_ref):
    chans, rows = piece_ref.shape
    many = 32
    width = many * LANES
    row = lax.broadcasted_iota(jnp.int32, (LANES, 2 * LANES), 0)
    col = lax.broadcasted_iota(jnp.int32, (LANES, 2 * LANES), 1)
    mask = jnp.where(row < col, 1.0, 0.0).astype(jnp.bfloat16)
    mask2 = jnp.concatenate([mask, mask], axis=0)

    def step(n, carry):
        at = pl.multiple_of(n * width, width)
        x = piece_ref[:, pl.ds(at, width)]
        x = jnp.concatenate([x[:, j * LANES : (j + 1) * LANES] for j in range(many)], axis=0)
        high = x.astype(jnp.bfloat16)
        rest = x - high.astype(jnp.float32)
        mid = rest.astype(jnp.bfloat16)
        low = (rest - mid.astype(jnp.float32)).astype(jnp.bfloat16)
        both = jnp.concatenate([high, mid], axis=1)
        res = jnp.dot(both, mask2, preferred_element_type=jnp.float32)
        res = res + jnp.dot(low, mask, preferred_element_type=jnp.float32)
        for j in range(many):
            part = res[j * chans : (j + 1) * chans]
            out_ref[:, pl.ds(pl.multiple_of(at + j * LANES, LANES), LANES)] = part[:, :LANES] + carry
            carry = carry + part[:, LANES:]
        return carry

    lax.fori_loop(0, rows // width, step, carry)


def scan_kernel(ks, with_carry, aliased, *refs):
    refs = list(refs)
    if aliased:
        refs.pop(0)
    pieces = [refs.pop(0) for _ in ks]
    apart = [refs.pop(0) for _ in range(sum(with_carry))]
    out_ref, held, sems = refs
    me = lax.axis_index("dev")
    copies = []
    for n, k in enumerate(ks):
        chans, rows = pieces[n].shape
        if with_carry[n]:
            carry = apart.pop(0)[...]
        else:
            last = pieces[n][:, rows - LANES :]
            carry = jnp.broadcast_to(last[:, LANES - 1 :], (chans, LANES))
        scan_piece(pieces[n], carry, held.at[n])
        start = pl.multiple_of((me ^ k) * chans, chans)
        copy = pltpu.make_async_copy(held.at[n], out_ref.at[pl.ds(start, chans), :], sems.at[n])
        copy.start()
        copies.append(copy)
    for copy in copies:
        copy.wait()


def scan(out, ks, pieces, apart):
    chans, rows = pieces[0].shape
    with_carry = [c is not None for c in apart]
    args = ([] if out is None else [out]) + list(pieces) + [c for c in apart if c is not None]
    return pl.pallas_call(
        functools.partial(scan_kernel, ks, with_carry, out is not None),
        out_shape=shape(chans * lax.axis_size("dev"), rows),
        in_specs=([] if out is None else [HBM]) + [VMEM] * (len(args) - (out is not None)),
        out_specs=HBM,
        scratch_shapes=[
            pltpu.VMEM((len(ks), chans, rows), jnp.float32),
            pltpu.SemaphoreType.DMA((len(ks),)),
        ],
        input_output_aliases={} if out is None else {0: 0},
        name="scan",
        **params(4, 20000000),
    )(*args)


def overlapped(a):
    count = lax.axis_size("dev")
    rows = a.shape[1] // count
    first, second, last = [2, 4], [3, 5], [6, 7, 1]
    p = dict(zip(first, grab(a, first, rows)))
    got = {k: swap(p[k], k) for k in first}
    late = second + last + [0]
    *pieces, total, chunk_sums = sums(a, first, [p[k] for k in first], late, rows)
    p.update(zip(late, pieces))
    got.update({k: swap(p[k], k) for k in second})
    groups = [shift_later(total, by) for by in range(1, lax.axis_size("grp"))]
    apart = first + second + [0]
    made = carries(chunk_sums, groups, last, [p[k] for k in last], apart)
    carry = dict(zip(apart, made[len(last) :]))
    got_carry = {k: swap(carry[k], k) for k in first + second}
    for k, piece in zip(last, made):
        got[k] = swap(piece, k)
    out = scan(None, [0], [p[0]], [carry[0]])
    for k in first + second:
        out = scan(out, [k], [got[k]], [got_carry[k]])
    for k in [1, 6, 7]:
        out = scan(out, [k], [got[k]], [None])
    return out


def plain(a):
    count = lax.axis_size("dev")
    chans, length = a.shape
    rows = length // count
    sums = jnp.sum(a.reshape(chans, count, rows), axis=2)
    carry = jnp.cumsum(sums, axis=1) - sums
    total = jnp.sum(sums, axis=1)
    for by in range(1, lax.axis_size("grp")):
        carry = carry + shift_later(total, by)[:, None]
    carry = lax.all_to_all(carry, "dev", split_axis=1, concat_axis=0, tiled=True)
    x = lax.all_to_all(a, "dev", split_axis=1, concat_axis=0, tiled=True)
    blocks = x.reshape(chans * count, rows // LANES, LANES)
    row = lax.broadcasted_iota(jnp.int32, (LANES, LANES), 0)
    col = lax.broadcasted_iota(jnp.int32, (LANES, LANES), 1)
    within = jnp.dot(
        blocks, (row < col).astype(jnp.float32), precision=lax.Precision.HIGHEST,
        preferred_element_type=jnp.float32,
    )
    block_sums = jnp.sum(blocks, axis=2)
    starts = jnp.cumsum(block_sums, axis=1) - block_sums + carry
    return (within + starts[:, :, None]).reshape(chans * count, rows)


def local(a):
    chans, length = a.shape
    fits = lax.axis_size("dev") == 8 and lax.axis_size("grp") > 1
    if fits and chans == 8 and length % (8 * 32 * LANES) == 0:
        return overlapped(a)
    return plain(a)


def solution(mesh):
    return jax.shard_map(
        local,
        mesh=mesh,
        in_specs=(P("dev", "grp"),),
        out_specs=P(None, ("grp", "dev")),
        check_vma=False,
    )
```

```python
import functools

import jax
import jax.numpy as jnp
from jax import lax
from jax.experimental import pallas as pl
from jax.experimental.pallas import tpu as pltpu
from jax.sharding import PartitionSpec as P


LANES = 128
VMEM = pl.BlockSpec(memory_space=pltpu.VMEM)
HBM = pl.BlockSpec(memory_space=pltpu.HBM)


def params(mib, flops):
    return {
        "compiler_params": pltpu.CompilerParams(vmem_limit_bytes=mib << 20),
        "cost_estimate": pl.CostEstimate(flops=flops, bytes_accessed=0, transcendentals=0),
    }


def shape(*dims):
    return jax.ShapeDtypeStruct(dims, jnp.float32)


def swap(value, k):
    count = lax.axis_size("dev")
    return lax.ppermute(value, "dev", [(i, i ^ k) for i in range(count)])


def shift_later(value, by):
    count = lax.axis_size("grp")
    return lax.ppermute(value, "grp", [(i, i + by) for i in range(count - by)])


def grab_kernel(ks, rows, a_ref, *refs):
    outs, sems = refs[: len(ks)], refs[-1]
    me = lax.axis_index("dev")
    copies = []
    for n, k in enumerate(ks):
        start = pl.multiple_of((me ^ k) * rows, rows)
        copy = pltpu.make_async_copy(a_ref.at[:, pl.ds(start, rows)], outs[n], sems.at[n])
        copy.start()
        copies.append(copy)
    for copy in copies:
        copy.wait()


def grab(a, ks, rows):
    chans = a.shape[0]
    return pl.pallas_call(
        functools.partial(grab_kernel, ks, rows),
        out_shape=[shape(chans, rows)] * len(ks),
        in_specs=[VMEM],
        out_specs=[VMEM] * len(ks),
        scratch_shapes=[pltpu.SemaphoreType.DMA((len(ks),))],
        name="grab",
        **params(8, 1000000),
    )(a)


def piece_sum(ref):
    chans, rows = ref.shape
    width = 8 * LANES

    def step(n, acc):
        at = pl.multiple_of(n * width, width)
        return acc + ref[:, pl.ds(at, width)]

    acc = lax.fori_loop(1, rows // width, step, ref[:, :width], unroll=True)
    total = acc[:, :LANES]
    for n in range(1, 8):
        total = total + acc[:, n * LANES : (n + 1) * LANES]
    return jnp.broadcast_to(jnp.sum(total, axis=1, keepdims=True), (chans, LANES))


def sums_kernel(late, rows, a_ref, *refs):
    late_refs = refs[: len(late)]
    total_ref, sums_ref, sems = refs[len(late) :]
    me = lax.axis_index("dev")
    chans = a_ref.shape[0]
    count = a_ref.shape[1] // rows
    copies = []
    for n, k in enumerate(late):
        start = pl.multiple_of((me ^ k) * rows, rows)
        copy = pltpu.make_async_copy(a_ref.at[:, pl.ds(start, rows)], late_refs[n], sems.at[n])
        copy.start()
        copies.append(copy)
    total = jnp.zeros((chans, LANES), jnp.float32)
    for e in range(count):
        part = piece_sum(a_ref.at[:, e * rows : (e + 1) * rows])
        total = total + part
        sums_ref[e * chans : (e + 1) * chans, :] = part
    total_ref[...] = total
    for copy in copies:
        copy.wait()


def sums(a, late, rows):
    chans, length = a.shape
    return pl.pallas_call(
        functools.partial(sums_kernel, late, rows),
        out_shape=[shape(chans, rows)] * len(late)
        + [shape(chans, LANES), shape(chans * (length // rows), LANES)],
        in_specs=[VMEM],
        out_specs=[VMEM] * (len(late) + 2),
        scratch_shapes=[pltpu.SemaphoreType.DMA((len(late),))],
        name="sums",
        **params(8, 40000000),
    )(a)


def carry_kernel(apart, inside, shifts, sums_ref, *refs):
    group_refs, refs = refs[:shifts], refs[shifts:]
    old_refs, refs = refs[: len(inside)], refs[len(inside) :]
    new_refs, apart_refs, carry_ref = refs[: len(inside)], refs[len(inside) : -1], refs[-1]
    me = lax.axis_index("dev")
    chans = group_refs[0].shape[0]
    count = sums_ref.shape[0] // chans
    carry = jnp.zeros((chans, LANES), jnp.float32)
    for ref in group_refs:
        carry = carry + ref[...]
    for e in range(count):
        carry_ref[e * chans : (e + 1) * chans, :] = carry
        carry = carry + sums_ref[e * chans : (e + 1) * chans, :]

    def carry_of(k):
        return carry_ref[pl.ds(pl.multiple_of((me ^ k) * chans, chans), chans), :]

    lane = lax.broadcasted_iota(jnp.int32, (chans, LANES), 1)
    for n, k in enumerate(inside):
        last = old_refs[n].shape[1] - LANES
        new_refs[n][:, last:] = jnp.where(lane == LANES - 1, carry_of(k), old_refs[n][:, last:])
    for n, k in enumerate(apart):
        apart_refs[n][...] = carry_of(k)


def carries(chunk_sums, groups, inside, pieces, apart):
    chans, rows = pieces[0].shape
    return pl.pallas_call(
        functools.partial(carry_kernel, apart, inside, len(groups)),
        out_shape=[shape(chans, rows)] * len(inside) + [shape(chans, LANES)] * len(apart),
        in_specs=[VMEM] * (1 + len(groups) + len(inside)),
        out_specs=[VMEM] * (len(inside) + len(apart)),
        scratch_shapes=[pltpu.VMEM(chunk_sums.shape, jnp.float32)],
        input_output_aliases={1 + len(groups) + n: n for n in range(len(inside))},
        name="carries",
        **params(8, 10000000),
    )(chunk_sums, *groups, *pieces)


def scan_piece(piece_ref, carry, out_ref):
    chans, rows = piece_ref.shape
    many = 32
    width = many * LANES
    row = lax.broadcasted_iota(jnp.int32, (LANES, 2 * LANES), 0)
    col = lax.broadcasted_iota(jnp.int32, (LANES, 2 * LANES), 1)
    mask = jnp.where(row < col, 1.0, 0.0).astype(jnp.bfloat16)
    mask2 = jnp.concatenate([mask, mask], axis=0)

    def step(n, carry):
        at = pl.multiple_of(n * width, width)
        x = piece_ref[:, pl.ds(at, width)]
        x = jnp.concatenate([x[:, j * LANES : (j + 1) * LANES] for j in range(many)], axis=0)
        high = x.astype(jnp.bfloat16)
        rest = x - high.astype(jnp.float32)
        mid = rest.astype(jnp.bfloat16)
        low = (rest - mid.astype(jnp.float32)).astype(jnp.bfloat16)
        both = jnp.concatenate([high, mid], axis=1)
        res = jnp.dot(both, mask2, preferred_element_type=jnp.float32)
        res = res + jnp.dot(low, mask, preferred_element_type=jnp.float32)
        for j in range(many):
            part = res[j * chans : (j + 1) * chans]
            out_ref[:, pl.ds(pl.multiple_of(at + j * LANES, LANES), LANES)] = part[:, :LANES] + carry
            carry = carry + part[:, LANES:]
        return carry

    lax.fori_loop(0, rows // width, step, carry)


def scan_kernel(ks, with_carry, aliased, *refs):
    refs = list(refs)
    if aliased:
        refs.pop(0)
    pieces = [refs.pop(0) for _ in ks]
    apart = [refs.pop(0) for _ in range(sum(with_carry))]
    out_ref, held, sems = refs
    me = lax.axis_index("dev")
    copies = []
    for n, k in enumerate(ks):
        chans, rows = pieces[n].shape
        if with_carry[n]:
            carry = apart.pop(0)[...]
        else:
            last = pieces[n][:, rows - LANES :]
            carry = jnp.broadcast_to(last[:, LANES - 1 :], (chans, LANES))
        scan_piece(pieces[n], carry, held.at[n])
        start = pl.multiple_of((me ^ k) * chans, chans)
        copy = pltpu.make_async_copy(held.at[n], out_ref.at[pl.ds(start, chans), :], sems.at[n])
        copy.start()
        copies.append(copy)
    for copy in copies:
        copy.wait()


def scan(out, ks, pieces, apart):
    chans, rows = pieces[0].shape
    with_carry = [c is not None for c in apart]
    args = ([] if out is None else [out]) + list(pieces) + [c for c in apart if c is not None]
    return pl.pallas_call(
        functools.partial(scan_kernel, ks, with_carry, out is not None),
        out_shape=shape(chans * lax.axis_size("dev"), rows),
        in_specs=([] if out is None else [HBM]) + [VMEM] * (len(args) - (out is not None)),
        out_specs=HBM,
        scratch_shapes=[
            pltpu.VMEM((len(ks), chans, rows), jnp.float32),
            pltpu.SemaphoreType.DMA((len(ks),)),
        ],
        input_output_aliases={} if out is None else {0: 0},
        name="scan",
        **params(4, 20000000),
    )(*args)


def overlapped(a):
    chans, length = a.shape
    rows = length // lax.axis_size("dev")
    me = lax.axis_index("dev")
    ahead, early, late = [4, 2], [5, 3], [6, 7, 1]
    p = {k: lax.dynamic_slice(a, (0, (me ^ k) * rows), (chans, rows)) for k in ahead}
    p.update(zip(early, grab(a, early, rows)))
    early = ahead + early
    got = {k: swap(p[k], k) for k in early}
    *pieces, total, chunk_sums = sums(a, late + [0], rows)
    p.update(zip(late + [0], pieces))
    groups = [shift_later(total, by) for by in range(1, lax.axis_size("grp"))]
    apart = early + [0]
    made = carries(chunk_sums, groups, late, [p[k] for k in late], apart)
    carry = dict(zip(apart, made[len(late) :]))
    got_carry = {k: swap(carry[k], k) for k in early}
    for k, piece in zip(late, made):
        got[k] = swap(piece, k)
    out = scan(None, [0], [p[0]], [carry[0]])
    for k in [2, 4, 3, 5]:
        out = scan(out, [k], [got[k]], [got_carry[k]])
    for k in [1, 6, 7]:
        out = scan(out, [k], [got[k]], [None])
    return out


def plain(a):
    count = lax.axis_size("dev")
    chans, length = a.shape
    rows = length // count
    sums = jnp.sum(a.reshape(chans, count, rows), axis=2)
    carry = jnp.cumsum(sums, axis=1) - sums
    total = jnp.sum(sums, axis=1)
    for by in range(1, lax.axis_size("grp")):
        carry = carry + shift_later(total, by)[:, None]
    carry = lax.all_to_all(carry, "dev", split_axis=1, concat_axis=0, tiled=True)
    x = lax.all_to_all(a, "dev", split_axis=1, concat_axis=0, tiled=True)
    blocks = x.reshape(chans * count, rows // LANES, LANES)
    row = lax.broadcasted_iota(jnp.int32, (LANES, LANES), 0)
    col = lax.broadcasted_iota(jnp.int32, (LANES, LANES), 1)
    within = jnp.dot(
        blocks, (row < col).astype(jnp.float32), precision=lax.Precision.HIGHEST,
        preferred_element_type=jnp.float32,
    )
    block_sums = jnp.sum(blocks, axis=2)
    starts = jnp.cumsum(block_sums, axis=1) - block_sums + carry
    return (within + starts[:, :, None]).reshape(chans * count, rows)


def local(a):
    chans, length = a.shape
    fits = lax.axis_size("dev") == 8 and lax.axis_size("grp") > 1
    if fits and chans == 8 and length % (8 * 32 * LANES) == 0:
        return overlapped(a)
    return plain(a)


def solution(mesh):
    return jax.shard_map(
        local,
        mesh=mesh,
        in_specs=(P("dev", "grp"),),
        out_specs=P(None, ("grp", "dev")),
        check_vma=False,
    )
```

```python
import functools

import jax
import jax.numpy as jnp
from jax import lax
from jax.experimental import pallas as pl
from jax.experimental.pallas import tpu as pltpu
from jax.sharding import PartitionSpec as P


LANES = 128
VMEM = pl.BlockSpec(memory_space=pltpu.VMEM)
HBM = pl.BlockSpec(memory_space=pltpu.HBM)


def params(mib, flops):
    return {
        "compiler_params": pltpu.CompilerParams(vmem_limit_bytes=mib << 20),
        "cost_estimate": pl.CostEstimate(flops=flops, bytes_accessed=0, transcendentals=0),
    }


def shape(*dims):
    return jax.ShapeDtypeStruct(dims, jnp.float32)


X_OR_Y, Y_OR_X = (2, 4), (4, 2)
X_OTHER, Y_OTHER, DIAGONAL, DIAGONAL_OTHER, CORE, SELF = ((k, k) for k in (3, 5, 6, 7, 1, 0))


def partner(k):
    me = lax.axis_index("dev")
    return me ^ (k[0] + (me & 1) * (k[1] - k[0]))


def swap(value, k):
    count = lax.axis_size("dev")
    return lax.ppermute(value, "dev", [(i, i ^ k[i & 1]) for i in range(count)])


def shift_later(value, by):
    count = lax.axis_size("grp")
    return lax.ppermute(value, "grp", [(i, i + by) for i in range(count - by)])


def fetch(a_ref, ks, refs, sems):
    rows = a_ref.shape[1] // lax.axis_size("dev")
    copies = []
    for n, k in enumerate(ks):
        start = pl.multiple_of(partner(k) * rows, rows)
        copy = pltpu.make_async_copy(a_ref.at[:, pl.ds(start, rows)], refs[n], sems.at[n])
        copy.start()
        copies.append(copy)
    return copies


def grab_kernel(ks, a_ref, *refs):
    for copy in fetch(a_ref, ks, refs[:-1], refs[-1]):
        copy.wait()


def grab(a, ks):
    chans, length = a.shape
    return pl.pallas_call(
        functools.partial(grab_kernel, ks),
        out_shape=[shape(chans, length // lax.axis_size("dev"))] * len(ks),
        in_specs=[HBM],
        out_specs=[VMEM] * len(ks),
        scratch_shapes=[pltpu.SemaphoreType.DMA((len(ks),))],
        name="grab",
        **params(8, 1000000),
    )(a)


def piece_sum(ref):
    chans, rows = ref.shape
    width = 8 * LANES

    def step(n, acc):
        at = pl.multiple_of(n * width, width)
        return acc + ref[:, pl.ds(at, width)]

    acc = lax.fori_loop(1, rows // width, step, ref[:, :width], unroll=True)
    total = acc[:, :LANES]
    for n in range(1, 8):
        total = total + acc[:, n * LANES : (n + 1) * LANES]
    return jnp.broadcast_to(jnp.sum(total, axis=1, keepdims=True), (chans, LANES))


def sums_kernel(ahead, rest, a_ref, *refs):
    ahead_refs, refs = refs[: len(ahead)], refs[len(ahead) :]
    rest_refs, (total_ref, sums_ref, sems) = refs[: len(rest)], refs[len(rest) :]
    chans = a_ref.shape[0]
    copies = fetch(a_ref, rest, rest_refs, sems)
    total = jnp.zeros((chans, LANES), jnp.float32)
    for k, ref, copy in zip(ahead + rest, ahead_refs + rest_refs, [None] * len(ahead) + copies):
        if copy is not None:
            copy.wait()
        this = piece_sum(ref)
        total = total + this
        sums_ref[pl.ds(pl.multiple_of(partner(k) * chans, chans), chans), :] = this
    total_ref[...] = total


def sums(a, ahead, pieces, rest):
    chans, rows = pieces[0].shape
    return pl.pallas_call(
        functools.partial(sums_kernel, ahead, rest),
        out_shape=[shape(chans, rows)] * len(rest)
        + [shape(chans, LANES), shape(chans * lax.axis_size("dev"), LANES)],
        in_specs=[HBM] + [VMEM] * len(ahead),
        out_specs=[VMEM] * (len(rest) + 2),
        scratch_shapes=[pltpu.SemaphoreType.DMA((len(rest),))],
        name="sums",
        **params(8, 40000000),
    )(a, *pieces)


def carry_kernel(apart, inside, shifts, sums_ref, *refs):
    group_refs, refs = refs[:shifts], refs[shifts:]
    old_refs, refs = refs[: len(inside)], refs[len(inside) :]
    new_refs, apart_refs, carry_ref = refs[: len(inside)], refs[len(inside) : -1], refs[-1]
    chans = group_refs[0].shape[0]
    count = sums_ref.shape[0] // chans
    carry = jnp.zeros((chans, LANES), jnp.float32)
    for ref in group_refs:
        carry = carry + ref[...]
    for e in range(count):
        carry_ref[e * chans : (e + 1) * chans, :] = carry
        carry = carry + sums_ref[e * chans : (e + 1) * chans, :]

    def carry_of(k):
        return carry_ref[pl.ds(pl.multiple_of(partner(k) * chans, chans), chans), :]

    lane = lax.broadcasted_iota(jnp.int32, (chans, LANES), 1)
    for n, k in enumerate(inside):
        at = old_refs[n].shape[1] - LANES
        new_refs[n][:, at:] = jnp.where(lane == LANES - 1, carry_of(k), old_refs[n][:, at:])
    for n, k in enumerate(apart):
        apart_refs[n][...] = carry_of(k)


def carries(chunk_sums, groups, inside, pieces, apart):
    chans = pieces[0].shape[0]
    return pl.pallas_call(
        functools.partial(carry_kernel, apart, inside, len(groups)),
        out_shape=[shape(*piece.shape) for piece in pieces] + [shape(chans, LANES)] * len(apart),
        in_specs=[VMEM] * (1 + len(groups) + len(inside)),
        out_specs=[VMEM] * (len(inside) + len(apart)),
        scratch_shapes=[pltpu.VMEM(chunk_sums.shape, jnp.float32)],
        input_output_aliases={1 + len(groups) + n: n for n in range(len(inside))},
        name="carries",
        **params(8, 10000000),
    )(chunk_sums, *groups, *pieces)


STEP = 32


def scan_piece(piece_ref, carry, held_ref, done):
    chans, rows = piece_ref.shape
    many = STEP
    width = many * LANES
    row = lax.broadcasted_iota(jnp.int32, (LANES, 2 * LANES), 0)
    col = lax.broadcasted_iota(jnp.int32, (LANES, 2 * LANES), 1)
    mask = jnp.where(row < col, 1.0, 0.0).astype(jnp.bfloat16)
    mask2 = jnp.concatenate([mask, mask], axis=0)
    for at in range(0, rows, width):
        x = piece_ref[:, at : at + width]
        x = jnp.concatenate([x[:, j * LANES : (j + 1) * LANES] for j in range(many)], axis=0)
        high = x.astype(jnp.bfloat16)
        rest = x - high.astype(jnp.float32)
        mid = rest.astype(jnp.bfloat16)
        low = (rest - mid.astype(jnp.float32)).astype(jnp.bfloat16)
        both = jnp.concatenate([high, mid], axis=1)
        res = jnp.dot(both, mask2, preferred_element_type=jnp.float32)
        res = res + jnp.dot(low, mask, preferred_element_type=jnp.float32)
        for j in range(many):
            part = res[j * chans : (j + 1) * chans]
            start = at + j * LANES
            held_ref[:, start : start + LANES] = part[:, :LANES] + carry
            carry = carry + part[:, LANES:]
        done(at, width)


def scan_kernel(k, aliased, apart, *refs):
    piece_ref, *refs = refs[aliased:]
    chans, rows = piece_ref.shape
    if apart:
        carry_ref, *refs = refs
        carry = carry_ref[...]
    else:
        last = piece_ref[:, rows - LANES :]
        carry = jnp.broadcast_to(last[:, LANES - 1 :], last.shape)
    out_ref, held_ref, sems = refs
    start = pl.multiple_of(partner(k) * chans, chans)
    copies = []

    def copy_out(at, width):
        target = out_ref.at[pl.ds(start, chans), pl.ds(at, width)]
        copies.append(pltpu.make_async_copy(held_ref.at[:, pl.ds(at, width)], target, sems.at[at // width]))
        copies[-1].start()

    scan_piece(piece_ref, carry, held_ref, copy_out)
    for copy in copies:
        copy.wait()


def scan(out, k, piece, carry=None):
    chans, rows = piece.shape
    inputs = [piece] if carry is None else [piece, carry]
    before = [] if out is None else [out]
    return pl.pallas_call(
        functools.partial(scan_kernel, k, len(before), carry is not None),
        out_shape=shape(chans * lax.axis_size("dev"), rows),
        in_specs=[HBM] * len(before) + [VMEM] * len(inputs),
        out_specs=HBM,
        scratch_shapes=[
            pltpu.VMEM((chans, rows), jnp.float32),
            pltpu.SemaphoreType.DMA((rows // (STEP * LANES),)),
        ],
        input_output_aliases={0: 0} if before else {},
        name="scan",
        **params(8, 20000000),
    )(*before, *inputs)


def scan_ahead_kernel(piece_ref, carry_ref, out_ref):
    scan_piece(piece_ref, carry_ref[...], out_ref, lambda at, width: None)


def scan_ahead(piece, carry):
    return pl.pallas_call(
        scan_ahead_kernel,
        out_shape=shape(*piece.shape),
        in_specs=[VMEM] * 2,
        out_specs=VMEM,
        name="scan_ahead",
        **params(8, 20000000),
    )(piece, carry)


def place_kernel(k, _, piece_ref, out_ref, sem):
    chans = piece_ref.shape[0]
    start = pl.multiple_of(partner(k) * chans, chans)
    copy = pltpu.make_async_copy(piece_ref, out_ref.at[pl.ds(start, chans), :], sem)
    copy.start()
    copy.wait()


def place(out, k, piece):
    return pl.pallas_call(
        functools.partial(place_kernel, k),
        out_shape=shape(*out.shape),
        in_specs=[HBM, VMEM],
        out_specs=HBM,
        scratch_shapes=[pltpu.SemaphoreType.DMA],
        input_output_aliases={0: 0},
        name="place",
        **params(8, 1000000),
    )(out, piece)


AHEAD, EARLY = [X_OR_Y, Y_OR_X], [Y_OTHER, X_OTHER]
LATE, LAST = [DIAGONAL, CORE], DIAGONAL_OTHER


def overlapped(a):
    a = pltpu.with_memory_space_constraint(a, pltpu.HBM)
    piece = dict(zip(AHEAD, grab(a, AHEAD)))
    rest = EARLY + LATE + [LAST, SELF]
    *pieces, total, chunk_sums = sums(a, AHEAD, [piece[k] for k in AHEAD], rest)
    piece.update(zip(rest, pieces))
    got = {k: swap(piece[k], k) for k in AHEAD + EARLY}
    groups = [shift_later(total, by) for by in range(1, lax.axis_size("grp"))]
    apart = AHEAD + EARLY + [LAST, SELF]
    made = carries(chunk_sums, groups, LATE, [piece[k] for k in LATE], apart)
    carry = dict(zip(apart, made[len(LATE) :]))
    got_carry = {k: swap(carry[k], k) for k in AHEAD + EARLY}
    for k, value in zip(LATE, made):
        got[k] = swap(value, k)
    got[LAST] = swap(scan_ahead(piece[LAST], carry[LAST]), LAST)
    out = scan(None, SELF, piece[SELF], carry[SELF])
    for k in AHEAD + EARLY:
        out = scan(out, k, got[k], got_carry[k])
    for k in reversed(LATE):
        out = scan(out, k, got[k])
    return place(out, LAST, got[LAST])


def plain(a):
    count = lax.axis_size("dev")
    chans, length = a.shape
    rows = length // count
    sums = jnp.sum(a.reshape(chans, count, rows), axis=2)
    carry = jnp.cumsum(sums, axis=1) - sums
    total = jnp.sum(sums, axis=1)
    for by in range(1, lax.axis_size("grp")):
        carry = carry + shift_later(total, by)[:, None]
    carry = lax.all_to_all(carry, "dev", split_axis=1, concat_axis=0, tiled=True)
    x = lax.all_to_all(a, "dev", split_axis=1, concat_axis=0, tiled=True)
    blocks = x.reshape(chans * count, rows // LANES, LANES)
    row = lax.broadcasted_iota(jnp.int32, (LANES, LANES), 0)
    col = lax.broadcasted_iota(jnp.int32, (LANES, LANES), 1)
    within = jnp.dot(
        blocks, (row < col).astype(jnp.float32), precision=lax.Precision.HIGHEST,
        preferred_element_type=jnp.float32,
    )
    block_sums = jnp.sum(blocks, axis=2)
    starts = jnp.cumsum(block_sums, axis=1) - block_sums + carry
    return (within + starts[:, :, None]).reshape(chans * count, rows)


def local(a):
    chans, length = a.shape
    fits = lax.axis_size("dev") == 8 and lax.axis_size("grp") > 1
    if fits and chans == 8 and length % (8 * STEP * LANES) == 0:
        return overlapped(a)
    return plain(a)


def solution(mesh):
    return jax.shard_map(
        local,
        mesh=mesh,
        in_specs=(P("dev", "grp"),),
        out_specs=P(None, ("grp", "dev")),
        check_vma=False,
    )
```

```python
import functools

import jax
import jax.numpy as jnp
from jax import lax
from jax.experimental import pallas as pl
from jax.experimental.pallas import tpu as pltpu
from jax.sharding import PartitionSpec as P


LANES = 128
VMEM = pl.BlockSpec(memory_space=pltpu.VMEM)
HBM = pl.BlockSpec(memory_space=pltpu.HBM)


def params(mib, flops):
    return {
        "compiler_params": pltpu.CompilerParams(vmem_limit_bytes=mib << 20),
        "cost_estimate": pl.CostEstimate(flops=flops, bytes_accessed=0, transcendentals=0),
    }


def shape(*dims):
    return jax.ShapeDtypeStruct(dims, jnp.float32)


X_OR_Y, Y_OR_X = (2, 4), (4, 2)
X_OTHER, Y_OTHER, DIAGONAL, DIAGONAL_OTHER, CORE, SELF = ((k, k) for k in (3, 5, 6, 7, 1, 0))


def partner(k):
    me = lax.axis_index("dev")
    return me ^ (k[0] + (me & 1) * (k[1] - k[0]))


def swap(value, k):
    count = lax.axis_size("dev")
    return lax.ppermute(value, "dev", [(i, i ^ k[i & 1]) for i in range(count)])


def shift_later(value, by):
    count = lax.axis_size("grp")
    return lax.ppermute(value, "grp", [(i, i + by) for i in range(count - by)])


def fetch(a_ref, ks, refs, sems):
    rows = a_ref.shape[1] // lax.axis_size("dev")
    copies = []
    for n, k in enumerate(ks):
        start = pl.multiple_of(partner(k) * rows, rows)
        copy = pltpu.make_async_copy(a_ref.at[:, pl.ds(start, rows)], refs[n], sems.at[n])
        copy.start()
        copies.append(copy)
    return copies


def grab_kernel(ks, a_ref, *refs):
    for copy in fetch(a_ref, ks, refs[:-1], refs[-1]):
        copy.wait()


def grab(a, ks):
    chans, length = a.shape
    return pl.pallas_call(
        functools.partial(grab_kernel, ks),
        out_shape=[shape(chans, length // lax.axis_size("dev"))] * len(ks),
        in_specs=[HBM],
        out_specs=[VMEM] * len(ks),
        scratch_shapes=[pltpu.SemaphoreType.DMA((len(ks),))],
        name="grab",
        **params(8, 1000000),
    )(a)


def piece_sum(ref):
    chans, rows = ref.shape
    width = 8 * LANES

    def step(n, acc):
        at = pl.multiple_of(n * width, width)
        return acc + ref[:, pl.ds(at, width)]

    acc = lax.fori_loop(1, rows // width, step, ref[:, :width], unroll=True)
    total = acc[:, :LANES]
    for n in range(1, 8):
        total = total + acc[:, n * LANES : (n + 1) * LANES]
    return jnp.broadcast_to(jnp.sum(total, axis=1, keepdims=True), (chans, LANES))


def sums_kernel(ahead, rest, a_ref, *refs):
    ahead_refs, refs = refs[: len(ahead)], refs[len(ahead) :]
    rest_refs, (total_ref, sums_ref, sems) = refs[: len(rest)], refs[len(rest) :]
    chans = a_ref.shape[0]
    copies = fetch(a_ref, rest, rest_refs, sems)
    total = jnp.zeros((chans, LANES), jnp.float32)
    for k, ref, copy in zip(ahead + rest, ahead_refs + rest_refs, [None] * len(ahead) + copies):
        if copy is not None:
            copy.wait()
        this = piece_sum(ref)
        total = total + this
        sums_ref[pl.ds(pl.multiple_of(partner(k) * chans, chans), chans), :] = this
    total_ref[...] = total


def sums(a, ahead, pieces, rest):
    chans, rows = pieces[0].shape
    return pl.pallas_call(
        functools.partial(sums_kernel, ahead, rest),
        out_shape=[shape(chans, rows)] * len(rest)
        + [shape(chans, LANES), shape(chans * lax.axis_size("dev"), LANES)],
        in_specs=[HBM] + [VMEM] * len(ahead),
        out_specs=[VMEM] * (len(rest) + 2),
        scratch_shapes=[pltpu.SemaphoreType.DMA((len(rest),))],
        name="sums",
        **params(8, 40000000),
    )(a, *pieces)


def carry_kernel(apart, inside, shifts, sums_ref, *refs):
    group_refs, refs = refs[:shifts], refs[shifts:]
    old_refs, refs = refs[: len(inside)], refs[len(inside) :]
    new_refs, apart_refs, carry_ref = refs[: len(inside)], refs[len(inside) : -1], refs[-1]
    chans = group_refs[0].shape[0]
    count = sums_ref.shape[0] // chans
    carry = jnp.zeros((chans, LANES), jnp.float32)
    for ref in group_refs:
        carry = carry + ref[...]
    for e in range(count):
        carry_ref[e * chans : (e + 1) * chans, :] = carry
        carry = carry + sums_ref[e * chans : (e + 1) * chans, :]

    def carry_of(k):
        return carry_ref[pl.ds(pl.multiple_of(partner(k) * chans, chans), chans), :]

    lane = lax.broadcasted_iota(jnp.int32, (chans, LANES), 1)
    for n, k in enumerate(inside):
        at = old_refs[n].shape[1] - LANES
        new_refs[n][:, at:] = jnp.where(lane == LANES - 1, carry_of(k), old_refs[n][:, at:])
    for n, k in enumerate(apart):
        apart_refs[n][...] = carry_of(k)


def carries(chunk_sums, groups, inside, pieces, apart):
    chans = pieces[0].shape[0]
    return pl.pallas_call(
        functools.partial(carry_kernel, apart, inside, len(groups)),
        out_shape=[shape(*piece.shape) for piece in pieces] + [shape(chans, LANES)] * len(apart),
        in_specs=[VMEM] * (1 + len(groups) + len(inside)),
        out_specs=[VMEM] * (len(inside) + len(apart)),
        scratch_shapes=[pltpu.VMEM(chunk_sums.shape, jnp.float32)],
        input_output_aliases={1 + len(groups) + n: n for n in range(len(inside))},
        name="carries",
        **params(8, 10000000),
    )(chunk_sums, *groups, *pieces)


STEP = 32


def scan_piece(piece_ref, carry, held_ref, done):
    chans, rows = piece_ref.shape
    many = STEP
    width = many * LANES
    row = lax.broadcasted_iota(jnp.int32, (LANES, 2 * LANES), 0)
    col = lax.broadcasted_iota(jnp.int32, (LANES, 2 * LANES), 1)
    mask = jnp.where(row < col, 1.0, 0.0).astype(jnp.bfloat16)
    mask2 = jnp.concatenate([mask, mask], axis=0)
    for at in range(0, rows, width):
        x = piece_ref[:, at : at + width]
        x = jnp.concatenate([x[:, j * LANES : (j + 1) * LANES] for j in range(many)], axis=0)
        high = x.astype(jnp.bfloat16)
        rest = x - high.astype(jnp.float32)
        mid = rest.astype(jnp.bfloat16)
        low = (rest - mid.astype(jnp.float32)).astype(jnp.bfloat16)
        both = jnp.concatenate([high, mid], axis=1)
        res = jnp.dot(both, mask2, preferred_element_type=jnp.float32)
        res = res + jnp.dot(low, mask, preferred_element_type=jnp.float32)
        for j in range(many):
            part = res[j * chans : (j + 1) * chans]
            start = at + j * LANES
            held_ref[:, start : start + LANES] = part[:, :LANES] + carry
            carry = carry + part[:, LANES:]
        done(at, width)


def scan_kernel(k, aliased, apart, *refs):
    piece_ref, *refs = refs[aliased:]
    chans, rows = piece_ref.shape
    if apart:
        carry_ref, *refs = refs
        carry = carry_ref[...]
    else:
        last = piece_ref[:, rows - LANES :]
        carry = jnp.broadcast_to(last[:, LANES - 1 :], last.shape)
    out_ref, held_ref, sems = refs
    start = pl.multiple_of(partner(k) * chans, chans)
    copies = []

    def copy_out(at, width):
        target = out_ref.at[pl.ds(start, chans), pl.ds(at, width)]
        copies.append(pltpu.make_async_copy(held_ref.at[:, pl.ds(at, width)], target, sems.at[at // width]))
        copies[-1].start()

    scan_piece(piece_ref, carry, held_ref, copy_out)
    for copy in copies:
        copy.wait()


def scan(out, k, piece, carry=None):
    chans, rows = piece.shape
    inputs = [piece] if carry is None else [piece, carry]
    before = [] if out is None else [out]
    return pl.pallas_call(
        functools.partial(scan_kernel, k, len(before), carry is not None),
        out_shape=shape(chans * lax.axis_size("dev"), rows),
        in_specs=[HBM] * len(before) + [VMEM] * len(inputs),
        out_specs=HBM,
        scratch_shapes=[
            pltpu.VMEM((chans, rows), jnp.float32),
            pltpu.SemaphoreType.DMA((rows // (STEP * LANES),)),
        ],
        input_output_aliases={0: 0} if before else {},
        name="scan",
        **params(8, 20000000),
    )(*before, *inputs)


def scan_ahead_kernel(piece_ref, carry_ref, out_ref):
    scan_piece(piece_ref, carry_ref[...], out_ref, lambda at, width: None)


def scan_ahead(piece, carry):
    return pl.pallas_call(
        scan_ahead_kernel,
        out_shape=shape(*piece.shape),
        in_specs=[VMEM] * 2,
        out_specs=VMEM,
        name="scan_ahead",
        **params(8, 20000000),
    )(piece, carry)


def place_kernel(k, _, piece_ref, out_ref, sem):
    chans = piece_ref.shape[0]
    start = pl.multiple_of(partner(k) * chans, chans)
    copy = pltpu.make_async_copy(piece_ref, out_ref.at[pl.ds(start, chans), :], sem)
    copy.start()
    copy.wait()


def place(out, k, piece):
    return pl.pallas_call(
        functools.partial(place_kernel, k),
        out_shape=shape(*out.shape),
        in_specs=[HBM, VMEM],
        out_specs=HBM,
        scratch_shapes=[pltpu.SemaphoreType.DMA],
        input_output_aliases={0: 0},
        name="place",
        **params(8, 1000000),
    )(out, piece)


AHEAD, EARLY = [X_OR_Y, Y_OR_X], [Y_OTHER, X_OTHER, DIAGONAL]
LATE, LAST = [CORE], DIAGONAL_OTHER


def overlapped(a):
    a = pltpu.with_memory_space_constraint(a, pltpu.HBM)
    piece = dict(zip(AHEAD, grab(a, AHEAD)))
    rest = EARLY + LATE + [LAST, SELF]
    *pieces, total, chunk_sums = sums(a, AHEAD, [piece[k] for k in AHEAD], rest)
    piece.update(zip(rest, pieces))
    got = {k: swap(piece[k], k) for k in AHEAD + EARLY}
    groups = [shift_later(total, by) for by in range(1, lax.axis_size("grp"))]
    apart = AHEAD + EARLY + [LAST, SELF]
    made = carries(chunk_sums, groups, LATE, [piece[k] for k in LATE], apart)
    carry = dict(zip(apart, made[len(LATE) :]))
    got_carry = {k: swap(carry[k], k) for k in AHEAD + EARLY}
    for k, value in zip(LATE, made):
        got[k] = swap(value, k)
    got[LAST] = swap(scan_ahead(piece[LAST], carry[LAST]), LAST)
    out = scan(None, SELF, piece[SELF], carry[SELF])
    for k in LATE:
        out = scan(out, k, got[k])
    for k in AHEAD + EARLY:
        out = scan(out, k, got[k], got_carry[k])
    return place(out, LAST, got[LAST])


def plain(a):
    count = lax.axis_size("dev")
    chans, length = a.shape
    rows = length // count
    sums = jnp.sum(a.reshape(chans, count, rows), axis=2)
    carry = jnp.cumsum(sums, axis=1) - sums
    total = jnp.sum(sums, axis=1)
    for by in range(1, lax.axis_size("grp")):
        carry = carry + shift_later(total, by)[:, None]
    carry = lax.all_to_all(carry, "dev", split_axis=1, concat_axis=0, tiled=True)
    x = lax.all_to_all(a, "dev", split_axis=1, concat_axis=0, tiled=True)
    blocks = x.reshape(chans * count, rows // LANES, LANES)
    row = lax.broadcasted_iota(jnp.int32, (LANES, LANES), 0)
    col = lax.broadcasted_iota(jnp.int32, (LANES, LANES), 1)
    within = jnp.dot(
        blocks, (row < col).astype(jnp.float32), precision=lax.Precision.HIGHEST,
        preferred_element_type=jnp.float32,
    )
    block_sums = jnp.sum(blocks, axis=2)
    starts = jnp.cumsum(block_sums, axis=1) - block_sums + carry
    return (within + starts[:, :, None]).reshape(chans * count, rows)


def local(a):
    chans, length = a.shape
    fits = lax.axis_size("dev") == 8 and lax.axis_size("grp") > 1
    if fits and chans == 8 and length % (8 * STEP * LANES) == 0:
        return overlapped(a)
    return plain(a)


def solution(mesh):
    return jax.shard_map(
        local,
        mesh=mesh,
        in_specs=(P("dev", "grp"),),
        out_specs=P(None, ("grp", "dev")),
        check_vma=False,
    )
```

```python
import functools

import jax
import jax.numpy as jnp
from jax import lax
from jax.experimental import pallas as pl
from jax.experimental.pallas import tpu as pltpu
from jax.sharding import PartitionSpec as P


LANES = 128
VMEM = pl.BlockSpec(memory_space=pltpu.VMEM)
HBM = pl.BlockSpec(memory_space=pltpu.HBM)


def params(mib, flops):
    return {
        "compiler_params": pltpu.CompilerParams(vmem_limit_bytes=mib << 20),
        "cost_estimate": pl.CostEstimate(flops=flops, bytes_accessed=0, transcendentals=0),
    }


def shape(*dims):
    return jax.ShapeDtypeStruct(dims, jnp.float32)


Y, X = (4, 4), (2, 2)
X_OTHER, Y_OTHER, DIAGONAL, DIAGONAL_OTHER, CORE, SELF = ((k, k) for k in (3, 5, 6, 7, 1, 0))


def partner(k):
    me = lax.axis_index("dev")
    return me ^ (k[0] + (me & 1) * (k[1] - k[0]))


def swap(value, k):
    count = lax.axis_size("dev")
    return lax.ppermute(value, "dev", [(i, i ^ k[i & 1]) for i in range(count)])


def shift_later(value, by):
    count = lax.axis_size("grp")
    return lax.ppermute(value, "grp", [(i, i + by) for i in range(count - by)])


def fetch(a_ref, ks, refs, sems):
    rows = a_ref.shape[1] // lax.axis_size("dev")
    copies = []
    for n, k in enumerate(ks):
        start = pl.multiple_of(partner(k) * rows, rows)
        copy = pltpu.make_async_copy(a_ref.at[:, pl.ds(start, rows)], refs[n], sems.at[n])
        copy.start()
        copies.append(copy)
    return copies


def grab_kernel(ks, a_ref, *refs):
    for copy in fetch(a_ref, ks, refs[:-1], refs[-1]):
        copy.wait()


def grab(a, ks):
    chans, length = a.shape
    return pl.pallas_call(
        functools.partial(grab_kernel, ks),
        out_shape=[shape(chans, length // lax.axis_size("dev"))] * len(ks),
        in_specs=[HBM],
        out_specs=[VMEM] * len(ks),
        scratch_shapes=[pltpu.SemaphoreType.DMA((len(ks),))],
        name="grab",
        **params(8, 1000000),
    )(a)


def piece_sum(ref):
    chans, rows = ref.shape
    width = 8 * LANES

    def step(n, acc):
        at = pl.multiple_of(n * width, width)
        return acc + ref[:, pl.ds(at, width)]

    acc = lax.fori_loop(1, rows // width, step, ref[:, :width], unroll=True)
    total = acc[:, :LANES]
    for n in range(1, 8):
        total = total + acc[:, n * LANES : (n + 1) * LANES]
    return jnp.broadcast_to(jnp.sum(total, axis=1, keepdims=True), (chans, LANES))


def sums_kernel(ahead, rest, a_ref, *refs):
    ahead_refs, refs = refs[: len(ahead)], refs[len(ahead) :]
    rest_refs, (total_ref, sums_ref, sems) = refs[: len(rest)], refs[len(rest) :]
    chans = a_ref.shape[0]
    copies = fetch(a_ref, rest, rest_refs, sems)
    total = jnp.zeros((chans, LANES), jnp.float32)
    for k, ref, copy in zip(ahead + rest, ahead_refs + rest_refs, [None] * len(ahead) + copies):
        if copy is not None:
            copy.wait()
        this = piece_sum(ref)
        total = total + this
        sums_ref[pl.ds(pl.multiple_of(partner(k) * chans, chans), chans), :] = this
    total_ref[...] = total


def sums(a, ahead, pieces, rest):
    chans, rows = pieces[0].shape
    return pl.pallas_call(
        functools.partial(sums_kernel, ahead, rest),
        out_shape=[shape(chans, rows)] * len(rest)
        + [shape(chans, LANES), shape(chans * lax.axis_size("dev"), LANES)],
        in_specs=[HBM] + [VMEM] * len(ahead),
        out_specs=[VMEM] * (len(rest) + 2),
        scratch_shapes=[pltpu.SemaphoreType.DMA((len(rest),))],
        name="sums",
        **params(8, 40000000),
    )(a, *pieces)


def carry_kernel(apart, inside, shifts, sums_ref, *refs):
    group_refs, refs = refs[:shifts], refs[shifts:]
    old_refs, refs = refs[: len(inside)], refs[len(inside) :]
    new_refs, apart_refs, carry_ref = refs[: len(inside)], refs[len(inside) : -1], refs[-1]
    chans = group_refs[0].shape[0]
    count = sums_ref.shape[0] // chans
    carry = jnp.zeros((chans, LANES), jnp.float32)
    for ref in group_refs:
        carry = carry + ref[...]
    for e in range(count):
        carry_ref[e * chans : (e + 1) * chans, :] = carry
        carry = carry + sums_ref[e * chans : (e + 1) * chans, :]

    def carry_of(k):
        return carry_ref[pl.ds(pl.multiple_of(partner(k) * chans, chans), chans), :]

    lane = lax.broadcasted_iota(jnp.int32, (chans, LANES), 1)
    for n, k in enumerate(inside):
        at = old_refs[n].shape[1] - LANES
        new_refs[n][:, at:] = jnp.where(lane == LANES - 1, carry_of(k), old_refs[n][:, at:])
    for n, k in enumerate(apart):
        apart_refs[n][...] = carry_of(k)


def carries(chunk_sums, groups, inside, pieces, apart):
    chans = pieces[0].shape[0]
    return pl.pallas_call(
        functools.partial(carry_kernel, apart, inside, len(groups)),
        out_shape=[shape(*piece.shape) for piece in pieces] + [shape(chans, LANES)] * len(apart),
        in_specs=[VMEM] * (1 + len(groups) + len(inside)),
        out_specs=[VMEM] * (len(inside) + len(apart)),
        scratch_shapes=[pltpu.VMEM(chunk_sums.shape, jnp.float32)],
        input_output_aliases={1 + len(groups) + n: n for n in range(len(inside))},
        name="carries",
        **params(8, 10000000),
    )(chunk_sums, *groups, *pieces)


STEP = 32


def scan_piece(piece_ref, carry, held_ref, done):
    chans, rows = piece_ref.shape
    many = STEP
    width = many * LANES
    row = lax.broadcasted_iota(jnp.int32, (LANES, 2 * LANES), 0)
    col = lax.broadcasted_iota(jnp.int32, (LANES, 2 * LANES), 1)
    mask = jnp.where(row < col, 1.0, 0.0).astype(jnp.bfloat16)
    mask2 = jnp.concatenate([mask, mask], axis=0)
    for at in range(0, rows, width):
        x = piece_ref[:, at : at + width]
        x = jnp.concatenate([x[:, j * LANES : (j + 1) * LANES] for j in range(many)], axis=0)
        high = x.astype(jnp.bfloat16)
        rest = x - high.astype(jnp.float32)
        mid = rest.astype(jnp.bfloat16)
        low = (rest - mid.astype(jnp.float32)).astype(jnp.bfloat16)
        both = jnp.concatenate([high, mid], axis=1)
        res = jnp.dot(both, mask2, preferred_element_type=jnp.float32)
        res = res + jnp.dot(low, mask, preferred_element_type=jnp.float32)
        for j in range(many):
            part = res[j * chans : (j + 1) * chans]
            start = at + j * LANES
            held_ref[:, start : start + LANES] = part[:, :LANES] + carry
            carry = carry + part[:, LANES:]
        done(at, width)


def scan_kernel(k, aliased, apart, *refs):
    piece_ref, *refs = refs[aliased:]
    chans, rows = piece_ref.shape
    if apart:
        carry_ref, *refs = refs
        carry = carry_ref[...]
    else:
        last = piece_ref[:, rows - LANES :]
        carry = jnp.broadcast_to(last[:, LANES - 1 :], last.shape)
    out_ref, held_ref, sems = refs
    start = pl.multiple_of(partner(k) * chans, chans)
    copies = []

    def copy_out(at, width):
        target = out_ref.at[pl.ds(start, chans), pl.ds(at, width)]
        copies.append(pltpu.make_async_copy(held_ref.at[:, pl.ds(at, width)], target, sems.at[at // width]))
        copies[-1].start()

    scan_piece(piece_ref, carry, held_ref, copy_out)
    for copy in copies:
        copy.wait()


def scan(out, k, piece, carry=None):
    chans, rows = piece.shape
    inputs = [piece] if carry is None else [piece, carry]
    before = [] if out is None else [out]
    return pl.pallas_call(
        functools.partial(scan_kernel, k, len(before), carry is not None),
        out_shape=shape(chans * lax.axis_size("dev"), rows),
        in_specs=[HBM] * len(before) + [VMEM] * len(inputs),
        out_specs=HBM,
        scratch_shapes=[
            pltpu.VMEM((chans, rows), jnp.float32),
            pltpu.SemaphoreType.DMA((rows // (STEP * LANES),)),
        ],
        input_output_aliases={0: 0} if before else {},
        name="scan",
        **params(8, 20000000),
    )(*before, *inputs)


def scan_ahead_kernel(piece_ref, carry_ref, main_ref, end_ref, held_ref):
    split = main_ref.shape[1]
    scan_piece(piece_ref, carry_ref[...], held_ref, lambda at, width: None)
    main_ref[...] = held_ref[:, :split]
    end_ref[...] = held_ref[:, split:]


def scan_ahead(piece, carry):
    chans, rows = piece.shape
    end = rows // 8
    return pl.pallas_call(
        scan_ahead_kernel,
        out_shape=[shape(chans, rows - end), shape(chans, end)],
        in_specs=[VMEM] * 2,
        out_specs=[VMEM] * 2,
        scratch_shapes=[pltpu.VMEM((chans, rows), jnp.float32)],
        name="scan_ahead",
        **params(8, 20000000),
    )(piece, carry)


def place_kernel(k, at, _, piece_ref, out_ref, sem):
    chans, width = piece_ref.shape
    start = pl.multiple_of(partner(k) * chans, chans)
    copy = pltpu.make_async_copy(piece_ref, out_ref.at[pl.ds(start, chans), pl.ds(at, width)], sem)
    copy.start()
    copy.wait()


def place(out, k, at, piece):
    return pl.pallas_call(
        functools.partial(place_kernel, k, at),
        out_shape=shape(*out.shape),
        in_specs=[HBM, VMEM],
        out_specs=HBM,
        scratch_shapes=[pltpu.SemaphoreType.DMA],
        input_output_aliases={0: 0},
        name="place",
        **params(8, 1000000),
    )(out, piece)


AHEAD, EARLY = [Y, X], [Y_OTHER, X_OTHER, DIAGONAL]
LATE, LAST = [CORE], DIAGONAL_OTHER


def overlapped(a):
    a = pltpu.with_memory_space_constraint(a, pltpu.HBM)
    piece = dict(zip(AHEAD, grab(a, AHEAD)))
    rest = EARLY + LATE + [LAST, SELF]
    *pieces, total, chunk_sums = sums(a, AHEAD, [piece[k] for k in AHEAD], rest)
    piece.update(zip(rest, pieces))
    got = {k: swap(piece[k], k) for k in AHEAD + EARLY}
    groups = [shift_later(total, by) for by in range(1, lax.axis_size("grp"))]
    apart = AHEAD + EARLY + [LAST, SELF]
    made = carries(chunk_sums, groups, LATE, [piece[k] for k in LATE], apart)
    carry = dict(zip(apart, made[len(LATE) :]))
    got_carry = {k: swap(carry[k], k) for k in AHEAD + EARLY}
    for k, value in zip(LATE, made):
        got[k] = swap(value, k)
    main, end = scan_ahead(piece[LAST], carry[LAST])
    main, end = swap(main, LAST), swap(end, LAST)
    out = scan(None, SELF, piece[SELF], carry[SELF])
    for k in LATE:
        out = scan(out, k, got[k])
    for k in AHEAD + EARLY:
        out = scan(out, k, got[k], got_carry[k])
    out = place(out, LAST, 0, main)
    return place(out, LAST, main.shape[1], end)


def plain(a):
    count = lax.axis_size("dev")
    chans, length = a.shape
    rows = length // count
    sums = jnp.sum(a.reshape(chans, count, rows), axis=2)
    carry = jnp.cumsum(sums, axis=1) - sums
    total = jnp.sum(sums, axis=1)
    for by in range(1, lax.axis_size("grp")):
        carry = carry + shift_later(total, by)[:, None]
    carry = lax.all_to_all(carry, "dev", split_axis=1, concat_axis=0, tiled=True)
    x = lax.all_to_all(a, "dev", split_axis=1, concat_axis=0, tiled=True)
    blocks = x.reshape(chans * count, rows // LANES, LANES)
    row = lax.broadcasted_iota(jnp.int32, (LANES, LANES), 0)
    col = lax.broadcasted_iota(jnp.int32, (LANES, LANES), 1)
    within = jnp.dot(
        blocks, (row < col).astype(jnp.float32), precision=lax.Precision.HIGHEST,
        preferred_element_type=jnp.float32,
    )
    block_sums = jnp.sum(blocks, axis=2)
    starts = jnp.cumsum(block_sums, axis=1) - block_sums + carry
    return (within + starts[:, :, None]).reshape(chans * count, rows)


def local(a):
    chans, length = a.shape
    fits = lax.axis_size("dev") == 8 and lax.axis_size("grp") > 1
    if fits and chans == 8 and length % (8 * STEP * LANES) == 0:
        return overlapped(a)
    return plain(a)


def solution(mesh):
    return jax.shard_map(
        local,
        mesh=mesh,
        in_specs=(P("dev", "grp"),),
        out_specs=P(None, ("grp", "dev")),
        check_vma=False,
    )
```
